32 devices in a mesh: gx: 2 (over x), gy: 4 (over z), band: 4 (over y, core).
Axes of the slice: x: 2, y: 2, z: 4, core: 2. Of those that a mesh axis runs over, the one named last changes fastest.
Arguments:
- orbitals: float32 [2, 16, 16, 48, 128], P(None, 'band', 'gx', 'gy'), may hold values from -3 to 3
- external: float32 [16, 48, 128], P('gx', 'gy'), may hold values from 2 to 6
Outputs:
- orbitals_next: float32 [2, 16, 16, 48, 128], P(None, 'band', 'gx', 'gy')
- potential_next: float32 [16, 48, 128], P('gx', 'gy')
The draws below stay inside these ranges and needn't reach their ends.
All inputs are finite; a program needn't handle non-finite values.
Results may differ from the reference program's by a relative error of at most 0.00002.
Values sent between devices are 32-bit elements; how exact they have to be, the bound alone decides.
A program may use at most 64 MiB of HBM per device.

```python
import jax
import jax.numpy as jnp
from jax import lax

NZ = 128
BANDS = 16
NX = 16
NY = 48


def draw_orbitals(key, part):
    shape = (2, BANDS, NX, NY, NZ)
    first_rows = jnp.arange(NX, dtype=jnp.int32)[:, None, None]
    second_rows = jnp.arange(NY, dtype=jnp.int32)[None, :, None]
    third_rows = jnp.arange(NZ, dtype=jnp.int32)[None, None, :]
    parity = (first_rows + second_rows + third_rows) % 2
    pattern = (1 - 2 * parity).astype(jnp.float32)
    amplitude = jax.random.uniform(key, shape, jnp.float32, 0.5, 2.0)
    return (amplitude * pattern[None, None]).astype(jnp.float32)


def level_of(stream_key, shape, split, low, high):
    def one(axis_at, blocks):
        heights = jax.random.uniform(jax.random.fold_in(jax.random.fold_in(stream_key, 6), axis_at), (blocks,), jnp.float32, low / len(split), high / len(split))
        return jnp.repeat(jnp.exp(heights), shape[axis_at] // blocks).reshape((-1,) + (1,) * (len(shape) - axis_at - 1))

    loudness = one(*split[0])
    for cut in split[1:]:
        loudness = loudness * one(*cut)
    return loudness


def setup_inputs(seed: int = 0) -> dict:
    streams_of = jax.random.split(jax.random.key(seed), 3)
    return {
        "orbitals": draw_orbitals(jax.random.fold_in(streams_of[2], 71), 0),
        "external": jnp.clip(2.0 + 4.0 * jax.random.uniform(streams_of[1], (NX, NY, NZ), jnp.float32) ** level_of(streams_of[1], (NX, NY, NZ), ((0, 2), (1, 4)), -0.2, 0.2), 2.0, 6.0),
    }


step_length = 0.15
exchange_coef = 0.7386
centre_weight = -2.5
near_weight = 4.0 / 3.0
far_weight = -1.0 / 12.0


def shifted(padded, which_axis, offset):
    dimensions = padded.ndim
    selector = []
    for position in range(dimensions):
        if position < dimensions - 3:
            selector.append(slice(None))
        elif position == which_axis:
            selector.append(slice(2 + offset, padded.shape[position] - 2 + offset))
        else:
            selector.append(slice(2, padded.shape[position] - 2))
    return padded[tuple(selector)]


def laplacian(padded):
    dimensions = padded.ndim
    centre = shifted(padded, dimensions - 1, 0)
    summed = 3.0 * centre_weight * centre
    for which_axis in range(dimensions - 3, dimensions):
        summed = summed + near_weight * (shifted(padded, which_axis, 1) + shifted(padded, which_axis, -1))
        summed = summed + far_weight * (shifted(padded, which_axis, 2) + shifted(padded, which_axis, -2))
    return summed


def taylor(values, apply_fn, interval):
    summed = values
    taylor_term = values
    for degree in range(1, 5):
        image = apply_fn(taylor_term)
        factor = interval / degree
        taylor_term = jnp.stack([factor * image[1], -factor * image[0]])
        summed = summed + taylor_term
    return summed


def hamiltonian(values, potential):
    padded = jnp.pad(values, ((0, 0), (2, 2), (2, 2), (2, 2)))
    return -0.5 * laplacian(padded) + potential * values


def reference(orbitals, external):
    density_now = jnp.sum(orbitals * orbitals, axis=(0, 1))
    potential_now = external - exchange_coef * jnp.cbrt(density_now)
    by_band = jnp.moveaxis(orbitals, 1, 0)

    def apply_now(values):
        return hamiltonian(values, potential_now)

    def predict(values):
        return taylor(values, apply_now, step_length)

    predicted = lax.map(predict, by_band)
    density_next = jnp.sum(predicted * predicted, axis=(0, 1))
    potential_next = external - exchange_coef * jnp.cbrt(density_next)

    def apply_next(values):
        return hamiltonian(values, potential_next)

    def finish(values):
        halfway = taylor(values, apply_now, step_length / 2)
        return taylor(halfway, apply_next, step_length / 2)

    result = lax.map(finish, by_band)
    return jnp.moveaxis(result, 0, 1), potential_next
```

```python
import functools

import jax
import jax.numpy as jnp
from jax import lax
from jax.experimental import pallas as pl
from jax.experimental.pallas import tpu as pltpu
from jax.sharding import PartitionSpec as P

step_length = 0.15
exchange_coef = 0.7386
centre_weight = -2.5
near_weight = 4.0 / 3.0
far_weight = -1.0 / 12.0
MESH = pl.DeviceIdType.MESH


def cube_root(d):
    guess = jnp.exp(jnp.log(d) * (1.0 / 3.0))
    better = guess - (guess - d / (guess * guess)) * (1.0 / 3.0)
    return jnp.where(d > 1e-30, better, guess)


def kernel(counts, orb_ref, ext_ref, out_ref, pot_ref, terms, pot_wide, density, x_send, x_recv, y_send, y_recv, d_send, d_recv):
    n_x, n_y, n_b = counts
    nx, ny, nf, nz = orb_ref.shape
    gx = lax.axis_index("gx")
    gy = lax.axis_index("gy")
    gb = lax.axis_index("band")
    has = {
        ("gx", 0): gx > 0,
        ("gx", 1): gx < n_x - 1,
        ("gy", 0): gy > 0,
        ("gy", 1): gy < n_y - 1,
    }
    place = {"gx": gx, "gy": gy}
    sides = [("gx", 0), ("gx", 1), ("gy", 0), ("gy", 1)]
    peers = [lax.rem(gb + j, n_b) for j in range(1, n_b)]

    def target(side):
        axis, up = side
        return {axis: place[axis] + (1 if up else -1)}

    barrier = pltpu.get_barrier_semaphore()
    partners = n_b - 1
    for side in sides:
        partners = partners + has[side].astype(jnp.int32)

        @pl.when(has[side])
        def _():
            pl.semaphore_signal(barrier, inc=1, device_id=target(side), device_id_type=MESH)

    for peer in peers:
        pl.semaphore_signal(barrier, inc=1, device_id={"band": peer}, device_id_type=MESH)
    pl.semaphore_wait(barrier, partners)

    def halo_copy(step, side):
        axis, up = side
        if axis == "gx":
            near = pl.ds(nx if up else 2, 2)
            land = pl.ds(0 if up else nx + 2, 2)
            src_index = (near, pl.ds(2, ny))
            dst = terms.at[step, land, pl.ds(2, ny)]
            sems = (x_send, x_recv)
        else:
            near = pl.ds(ny if up else 2, 2)
            land = pl.ds(0 if up else ny + 2, 2)
            src_index = (pl.ds(2, nx), near)
            dst = terms.at[step, pl.ds(2, nx), land]
            sems = (y_send, y_recv)
        if step == 0:
            begin = (nx if axis == "gx" else ny) - 2 if up else 0
            if axis == "gx":
                src = orb_ref.at[pl.ds(begin, 2)]
            else:
                src = orb_ref.at[:, pl.ds(begin, 2)]
        else:
            src = terms.at[(step,) + src_index]
        return pltpu.make_async_remote_copy(
            src_ref=src,
            dst_ref=dst,
            send_sem=sems[0].at[step, up],
            recv_sem=sems[1].at[step, 1 - up],
            device_id=target(side),
            device_id_type=MESH,
        )

    def start(step, axis):
        for up in (0, 1):

            @pl.when(has[(axis, up)])
            def _():
                halo_copy(step, (axis, up)).start()

    def await_halo(step, axis):
        for up in (0, 1):

            @pl.when(has[(axis, up)])
            def _():
                sems = (x_send, x_recv) if axis == "gx" else (y_send, y_recv)
                land = (
                    terms.at[step, pl.ds(nx + 2 if up else 0, 2), pl.ds(2, ny)]
                    if axis == "gx"
                    else terms.at[step, pl.ds(2, nx), pl.ds(ny + 2 if up else 0, 2)]
                )
                pltpu.make_async_remote_copy(
                    src_ref=land,
                    dst_ref=land,
                    send_sem=sems[0].at[step, up],
                    recv_sem=sems[1].at[step, up],
                    device_id=target((axis, up)),
                    device_id_type=MESH,
                ).wait_recv()

    def density_copy(which, j):
        return pltpu.make_async_remote_copy(
            src_ref=density.at[which, 0],
            dst_ref=density.at[which, n_b - 1 - j],
            send_sem=d_send.at[which, j],
            recv_sem=d_recv.at[which, n_b - 2 - j],
            device_id={"band": peers[j]},
            device_id_type=MESH,
        )

    def start_density(which):
        for j in range(n_b - 1):
            density_copy(which, j).start()

    def finish_potential(which):
        for slot in range(1, n_b):
            pltpu.make_async_remote_copy(
                src_ref=density.at[which, slot],
                dst_ref=density.at[which, slot],
                send_sem=d_send.at[which, slot - 1],
                recv_sem=d_recv.at[which, slot - 1],
                device_id={"band": peers[slot - 1]},
                device_id_type=MESH,
            ).wait_recv()

        def row(x, carry):
            total = density[which, 0, x]
            for slot in range(1, n_b):
                total = total + density[which, slot, x]
            pot = ext_ref[x] - exchange_coef * cube_root(total)
            if which == 1:
                pot_ref[x] = pot
            wide = pot - 1.5 * centre_weight
            for y in range(ny):
                pot_wide[x, y] = jnp.broadcast_to(wide[y : y + 1], (nf, nz))
            return carry

        lax.fori_loop(0, nx, row, 0)

    start(0, "gx")
    start(0, "gy")

    def load_row(x, carry):
        block = orb_ref[x]
        terms[0, x + 2, pl.ds(2, ny)] = block
        density[0, 0, x] = jnp.sum(block * block, axis=1)
        return carry

    lax.fori_loop(0, nx, load_row, 0)
    start_density(0)

    for side in sides:
        axis, up = side

        @pl.when(jnp.logical_not(has[side]))
        def _():
            def clear(step, carry):
                if axis == "gx":
                    shape = (2, ny, nf, nz)
                    terms[step, pl.ds(nx + 2 if up else 0, 2), pl.ds(2, ny)] = jnp.zeros(shape, jnp.float32)
                else:
                    shape = (nx, 2, nf, nz)
                    terms[step, pl.ds(2, nx), pl.ds(ny + 2 if up else 0, 2)] = jnp.zeros(shape, jnp.float32)
                return carry

            lax.fori_loop(0, 8, clear, 0)

    lane = lax.broadcasted_iota(jnp.int32, (nf, nz), 1)
    near = -0.5 * near_weight
    far = -0.5 * far_weight
    below1 = jnp.where(lane >= 1, near, 0.0)
    above1 = jnp.where(lane < nz - 1, near, 0.0)
    below2 = jnp.where(lane >= 2, far, 0.0)
    above2 = jnp.where(lane < nz - 2, far, 0.0)
    half = nf // 2
    field = lax.broadcasted_iota(jnp.int32, (nf, nz), 0)
    turn_sign = jnp.where(field < half, 1.0, -1.0)

    def turned(v):
        return jnp.concatenate([v[half:], v[:half]], axis=0) * turn_sign

    def image(step, x, y):
        c = terms[step, x + 2, y + 2]
        one = (terms[step, x + 1, y + 2] + terms[step, x + 3, y + 2]) + (
            terms[step, x + 2, y + 1] + terms[step, x + 2, y + 3]
        )
        two = (terms[step, x, y + 2] + terms[step, x + 4, y + 2]) + (
            terms[step, x + 2, y] + terms[step, x + 2, y + 4]
        )
        total = pot_wide[x, y] * c + near * one + far * two
        total = total + pltpu.roll(c, 1, 1) * below1 + pltpu.roll(c, nz - 1, 1) * above1
        return total + (pltpu.roll(c, 2, 1) * below2 + pltpu.roll(c, nz - 2, 1) * above2)

    def combine(parts, s):
        even = parts[0] + (-(s**2) / 2) * parts[2] + (s**4 / 24) * parts[4]
        odd = s * parts[1] + (-(s**3) / 6) * parts[3]
        return even + turned(odd)

    def advance(step, x_from, x_count):
        def row(i, carry):
            x = x_from + i
            squares = []
            for y in range(ny):
                new = image(step, x, y)
                if step % 4 < 3:
                    terms[step + 1, x + 2, y + 2] = new
                else:
                    parts = [terms[step - 3 + k, x + 2, y + 2] for k in range(4)] + [new]
                    if step == 3:
                        terms[4, x + 2, y + 2] = combine(parts, step_length / 2)
                        predicted = combine(parts, step_length)
                        squares.append(jnp.sum(predicted * predicted, axis=0, keepdims=True))
                    else:
                        out_ref[x, y] = combine(parts, step_length / 2)
            if step == 3:
                density[1, 0, x] = jnp.concatenate(squares, axis=0)
            return carry

        lax.fori_loop(0, x_count, row, 0)

    for step in range(8):
        if step % 4 == 0:
            finish_potential(step // 4)
        await_halo(step, "gx")
        await_halo(step, "gy")
        advance(step, 0, 2)
        advance(step, nx - 2, 2)
        if step < 7:
            start(step + 1, "gx")
        advance(step, 2, nx - 4)
        if step < 7:
            start(step + 1, "gy")
        if step == 3:
            start_density(1)

    for step in range(8):
        for side in sides:

            @pl.when(has[side])
            def _():
                halo_copy(step, side).wait_send()

    for which in (0, 1):
        for j in range(n_b - 1):
            density_copy(which, j).wait_send()


def body(counts, orbitals, external):
    parts, bands, nx, ny, nz = orbitals.shape
    nf = parts * bands
    fields = jnp.transpose(orbitals.reshape(nf, nx, ny, nz), (1, 2, 0, 3))
    n_b = counts[2]
    dma = pltpu.SemaphoreType.DMA
    result, potential = pl.pallas_call(
        functools.partial(kernel, counts),
        out_shape=(
            jax.ShapeDtypeStruct((nx, ny, nf, nz), jnp.float32),
            jax.ShapeDtypeStruct((nx, ny, nz), jnp.float32),
        ),
        in_specs=[pl.BlockSpec(memory_space=pltpu.VMEM)] * 2,
        out_specs=(pl.BlockSpec(memory_space=pltpu.VMEM),) * 2,
        scratch_shapes=[
            pltpu.VMEM((8, nx + 4, ny + 4, nf, nz), jnp.float32),
            pltpu.VMEM((nx, ny, nf, nz), jnp.float32),
            pltpu.VMEM((2, n_b, nx, ny, nz), jnp.float32),
            dma((8, 2)),
            dma((8, 2)),
            dma((8, 2)),
            dma((8, 2)),
            dma((2, n_b - 1)),
            dma((2, n_b - 1)),
        ],
        compiler_params=pltpu.CompilerParams(
            collective_id=0, has_side_effects=True, vmem_limit_bytes=40 * 1024 * 1024
        ),
    )(fields, external)
    result = jnp.transpose(result, (2, 0, 1, 3)).reshape(orbitals.shape)
    return (result, potential)


def solution(mesh):
    counts = (mesh.shape["gx"], mesh.shape["gy"], mesh.shape["band"])
    in_specs = (P(None, "band", "gx", "gy", None), P("gx", "gy", None))
    out_specs = (P(None, "band", "gx", "gy", None), P("gx", "gy", None))
    return jax.shard_map(
        functools.partial(body, counts), mesh=mesh, in_specs=in_specs, out_specs=out_specs, check_vma=False
    )
```

```python
import functools

import jax
import jax.numpy as jnp
from jax import lax
from jax.experimental import pallas as pl
from jax.experimental.pallas import tpu as pltpu
from jax.sharding import PartitionSpec as P

step_length = 0.15
exchange_coef = 0.7386
centre_weight = -2.5
near_weight = 4.0 / 3.0
far_weight = -1.0 / 12.0
MESH = pl.DeviceIdType.MESH


def cube_root(d):
    guess = jnp.exp(jnp.log(d) * (1.0 / 3.0))
    better = guess - (guess - d / (guess * guess)) * (1.0 / 3.0)
    return jnp.where(d > 1e-30, better, guess)


def kernel(counts, orb_ref, ext_ref, out_ref, pot_ref, terms, pot_wide, density, x_send, x_recv, y_send, y_recv, d_send, d_recv):
    n_x, n_y, n_b = counts
    nx, ny, nf, nz = orb_ref.shape
    gx = lax.axis_index("gx")
    gy = lax.axis_index("gy")
    gb = lax.axis_index("band")
    has = {
        ("gx", 0): gx > 0,
        ("gx", 1): gx < n_x - 1,
        ("gy", 0): gy > 0,
        ("gy", 1): gy < n_y - 1,
    }
    place = {"gx": gx, "gy": gy}
    sides = [("gx", 0), ("gx", 1), ("gy", 0), ("gy", 1)]
    peers = [lax.rem(gb + j, n_b) for j in range(1, n_b)]

    def target(side):
        axis, up = side
        return {axis: place[axis] + (1 if up else -1)}

    barrier = pltpu.get_barrier_semaphore()
    partners = n_b - 1
    for side in sides:
        partners = partners + has[side].astype(jnp.int32)

        @pl.when(has[side])
        def _():
            pl.semaphore_signal(barrier, inc=1, device_id=target(side), device_id_type=MESH)

    for peer in peers:
        pl.semaphore_signal(barrier, inc=1, device_id={"band": peer}, device_id_type=MESH)
    pl.semaphore_wait(barrier, partners)

    chunks = max(1, min(3, ny // 2))
    x_cuts = [(j * (ny // chunks), ny // chunks + (ny % chunks if j == chunks - 1 else 0)) for j in range(chunks)]
    y_cuts = [(0, 2), (nx - 2, 2), (2, nx - 4)]
    order = sorted(range(chunks), key=lambda j: 0 if j in (0, chunks - 1) else 1)
    sems = {"gx": (x_send, x_recv), "gy": (y_send, y_recv)}

    def cells(axis, edge, piece):
        if axis == "gx":
            return pl.ds(edge, 2), pl.ds(2 + x_cuts[piece][0], x_cuts[piece][1])
        return pl.ds(2 + y_cuts[piece][0], y_cuts[piece][1]), pl.ds(edge, 2)

    def send_copy(step, side, piece):
        axis, up = side
        extent = nx if axis == "gx" else ny
        if step > 0:
            src = terms.at[(step,) + cells(axis, extent if up else 2, piece)]
        elif axis == "gx":
            src = orb_ref.at[pl.ds(nx - 2 if up else 0, 2), pl.ds(*x_cuts[piece])]
        else:
            src = orb_ref.at[pl.ds(*y_cuts[piece]), pl.ds(ny - 2 if up else 0, 2)]
        return pltpu.make_async_remote_copy(
            src_ref=src,
            dst_ref=terms.at[(step,) + cells(axis, 0 if up else extent + 2, piece)],
            send_sem=sems[axis][0].at[step, up, piece],
            recv_sem=sems[axis][1].at[step, 1 - up, piece],
            device_id=target(side),
            device_id_type=MESH,
        )

    def start(step, side, piece):
        @pl.when(has[side])
        def _():
            send_copy(step, side, piece).start()

    def await_piece(step, side, piece):
        axis, up = side
        extent = nx if axis == "gx" else ny

        @pl.when(has[side])
        def _():
            land = terms.at[(step,) + cells(axis, extent + 2 if up else 0, piece)]
            pltpu.make_async_remote_copy(
                src_ref=land,
                dst_ref=land,
                send_sem=sems[axis][0].at[step, up, piece],
                recv_sem=sems[axis][1].at[step, up, piece],
                device_id=target(side),
                device_id_type=MESH,
            ).wait_recv()

    def density_copy(which, j, piece):
        rows = pl.ds(*y_cuts[piece])
        return pltpu.make_async_remote_copy(
            src_ref=density.at[which, 0, rows],
            dst_ref=density.at[which, n_b - 1 - j, rows],
            send_sem=d_send.at[which, j, piece],
            recv_sem=d_recv.at[which, n_b - 2 - j, piece],
            device_id={"band": peers[j]},
            device_id_type=MESH,
        )

    def start_density(which, piece):
        for j in range(n_b - 1):
            density_copy(which, j, piece).start()

    def finish_potential(which, piece):
        rows = pl.ds(*y_cuts[piece])
        for slot in range(1, n_b):
            pltpu.make_async_remote_copy(
                src_ref=density.at[which, slot, rows],
                dst_ref=density.at[which, slot, rows],
                send_sem=d_send.at[which, slot - 1, piece],
                recv_sem=d_recv.at[which, slot - 1, piece],
                device_id={"band": peers[slot - 1]},
                device_id_type=MESH,
            ).wait_recv()

        def row(i, carry):
            x = y_cuts[piece][0] + i
            total = density[which, 0, x]
            for slot in range(1, n_b):
                total = total + density[which, slot, x]
            pot = ext_ref[x] - exchange_coef * cube_root(total)
            if which == 1:
                pot_ref[x] = pot
            wide = pot - 1.5 * centre_weight
            for y in range(ny):
                pot_wide[x, y] = jnp.broadcast_to(wide[y : y + 1], (nf, nz))
            return carry

        lax.fori_loop(0, y_cuts[piece][1], row, 0)

    for j in order:
        for up in (0, 1):
            start(0, ("gx", up), j)
    for piece in range(3):
        for up in (0, 1):
            start(0, ("gy", up), piece)

    def load_row(x, carry):
        block = orb_ref[x]
        terms[0, x + 2, pl.ds(2, ny)] = block
        density[0, 0, x] = jnp.sum(block * block, axis=1)
        return carry

    for piece in range(3):
        lax.fori_loop(y_cuts[piece][0], sum(y_cuts[piece]), load_row, 0)
        start_density(0, piece)

    for side in sides:
        axis, up = side

        @pl.when(jnp.logical_not(has[side]))
        def _():
            def clear(step, carry):
                if axis == "gx":
                    shape = (2, ny, nf, nz)
                    terms[step, pl.ds(nx + 2 if up else 0, 2), pl.ds(2, ny)] = jnp.zeros(shape, jnp.float32)
                else:
                    shape = (nx, 2, nf, nz)
                    terms[step, pl.ds(2, nx), pl.ds(ny + 2 if up else 0, 2)] = jnp.zeros(shape, jnp.float32)
                return carry

            lax.fori_loop(0, 8, clear, 0)

    lane = lax.broadcasted_iota(jnp.int32, (nf, nz), 1)
    near = -0.5 * near_weight
    far = -0.5 * far_weight
    below1 = jnp.where(lane >= 1, near, 0.0)
    above1 = jnp.where(lane < nz - 1, near, 0.0)
    below2 = jnp.where(lane >= 2, far, 0.0)
    above2 = jnp.where(lane < nz - 2, far, 0.0)
    half = nf // 2
    field = lax.broadcasted_iota(jnp.int32, (nf, nz), 0)
    turn_sign = jnp.where(field < half, 1.0, -1.0)

    def turned(v):
        return jnp.concatenate([v[half:], v[:half]], axis=0) * turn_sign

    def image(step, x, y):
        c = terms[step, x + 2, y + 2]
        one = (terms[step, x + 1, y + 2] + terms[step, x + 3, y + 2]) + (
            terms[step, x + 2, y + 1] + terms[step, x + 2, y + 3]
        )
        two = (terms[step, x, y + 2] + terms[step, x + 4, y + 2]) + (
            terms[step, x + 2, y] + terms[step, x + 2, y + 4]
        )
        total = pot_wide[x, y] * c + near * one + far * two
        total = total + pltpu.roll(c, 1, 1) * below1 + pltpu.roll(c, nz - 1, 1) * above1
        return total + (pltpu.roll(c, 2, 1) * below2 + pltpu.roll(c, nz - 2, 1) * above2)

    def combine(parts, s):
        even = parts[0] + (-(s**2) / 2) * parts[2] + (s**4 / 24) * parts[4]
        odd = s * parts[1] + (-(s**3) / 6) * parts[3]
        return even + turned(odd)

    def advance(step, x_from, x_count, runs):
        def row(i, carry):
            x = x_from + i
            for y_from, y_count in runs:
                squares = []
                for y in range(y_from, y_from + y_count):
                    new = image(step, x, y)
                    if step % 4 < 3:
                        terms[step + 1, x + 2, y + 2] = new
                        continue
                    parts = [terms[step - 3 + k, x + 2, y + 2] for k in range(4)] + [new]
                    if step == 3:
                        terms[4, x + 2, y + 2] = combine(parts, step_length / 2)
                        predicted = combine(parts, step_length)
                        squares.append(jnp.sum(predicted * predicted, axis=0, keepdims=True))
                    else:
                        out_ref[x, y] = combine(parts, step_length / 2)
                if step == 3:
                    density[1, 0, x, pl.ds(y_from, y_count)] = jnp.concatenate(squares, axis=0)
            return carry

        lax.fori_loop(0, x_count, row, 0)

    for step in range(8):
        if step % 4 == 0:
            finish_potential(step // 4, 0)
            finish_potential(step // 4, 1)
        for j in order:
            edges = [("gy", up) for up, at in ((0, 0), (1, chunks - 1)) if at == j]
            for up in (0, 1):
                await_piece(step, ("gx", up), j)
            for side in edges:
                await_piece(step, side, 0)
                await_piece(step, side, 1)
            advance(step, 0, 2, [x_cuts[j]])
            advance(step, nx - 2, 2, [x_cuts[j]])
            if step < 7:
                for up in (0, 1):
                    start(step + 1, ("gx", up), j)
                for side in edges:
                    start(step + 1, side, 0)
                    start(step + 1, side, 1)
        if step == 3:
            start_density(1, 0)
            start_density(1, 1)
        if step % 4 == 0:
            finish_potential(step // 4, 2)
        await_piece(step, ("gy", 0), 2)
        await_piece(step, ("gy", 1), 2)
        advance(step, 2, nx - 4, [(0, 2), (ny - 2, 2)])
        if step < 7:
            start(step + 1, ("gy", 0), 2)
            start(step + 1, ("gy", 1), 2)
        advance(step, 2, nx - 4, [(2, ny - 4)])
        if step == 3:
            start_density(1, 2)

    for step in range(8):
        for side in sides:

            @pl.when(has[side])
            def _():
                for piece in range(chunks if side[0] == "gx" else 3):
                    send_copy(step, side, piece).wait_send()

    for which in (0, 1):
        for j in range(n_b - 1):
            for piece in range(3):
                density_copy(which, j, piece).wait_send()


def body(counts, orbitals, external):
    parts, bands, nx, ny, nz = orbitals.shape
    nf = parts * bands
    fields = jnp.transpose(orbitals.reshape(nf, nx, ny, nz), (1, 2, 0, 3))
    n_b = counts[2]
    dma = pltpu.SemaphoreType.DMA
    result, potential = pl.pallas_call(
        functools.partial(kernel, counts),
        out_shape=(
            jax.ShapeDtypeStruct((nx, ny, nf, nz), jnp.float32),
            jax.ShapeDtypeStruct((nx, ny, nz), jnp.float32),
        ),
        in_specs=[pl.BlockSpec(memory_space=pltpu.VMEM)] * 2,
        out_specs=(pl.BlockSpec(memory_space=pltpu.VMEM),) * 2,
        scratch_shapes=[
            pltpu.VMEM((8, nx + 4, ny + 4, nf, nz), jnp.float32),
            pltpu.VMEM((nx, ny, nf, nz), jnp.float32),
            pltpu.VMEM((2, n_b, nx, ny, nz), jnp.float32),
            dma((8, 2, 3)),
            dma((8, 2, 3)),
            dma((8, 2, 3)),
            dma((8, 2, 3)),
            dma((2, n_b - 1, 3)),
            dma((2, n_b - 1, 3)),
        ],
        compiler_params=pltpu.CompilerParams(
            collective_id=0, has_side_effects=True, vmem_limit_bytes=40 * 1024 * 1024
        ),
    )(fields, external)
    result = jnp.transpose(result, (2, 0, 1, 3)).reshape(orbitals.shape)
    return (result, potential)


def solution(mesh):
    counts = (mesh.shape["gx"], mesh.shape["gy"], mesh.shape["band"])
    in_specs = (P(None, "band", "gx", "gy", None), P("gx", "gy", None))
    out_specs = (P(None, "band", "gx", "gy", None), P("gx", "gy", None))
    return jax.shard_map(
        functools.partial(body, counts), mesh=mesh, in_specs=in_specs, out_specs=out_specs, check_vma=False
    )
```

```python
import functools

import jax
import jax.numpy as jnp
from jax import lax
from jax.experimental import pallas as pl
from jax.experimental.pallas import tpu as pltpu
from jax.sharding import PartitionSpec as P

step_length = 0.15
exchange_coef = 0.7386
centre_weight = -2.5
near_weight = 4.0 / 3.0
far_weight = -1.0 / 12.0
MESH = pl.DeviceIdType.MESH


def cube_root(d):
    guess = jnp.exp(jnp.log(d) * (1.0 / 3.0))
    better = guess - (guess - d / (guess * guess)) * (1.0 / 3.0)
    return jnp.where(d > 1e-30, better, guess)


def kernel(counts, orb_hbm, ext_hbm, out_ref, pot_ref, *scratch):
    terms = scratch[:8]
    orb_ref, ext_ref, pot_wide, density, in_sem, x_send, x_recv, y_send, y_recv, d_send, d_recv = scratch[8:]
    n_x, n_y, n_b = counts
    nf, ny, nx, nz = orb_ref.shape
    gx = lax.axis_index("gx")
    gy = lax.axis_index("gy")
    gb = lax.axis_index("band")
    has = {
        ("gx", 0): gx > 0,
        ("gx", 1): gx < n_x - 1,
        ("gy", 0): gy > 0,
        ("gy", 1): gy < n_y - 1,
    }
    place = {"gx": gx, "gy": gy}
    sides = [("gx", 0), ("gx", 1), ("gy", 0), ("gy", 1)]
    peers = [lax.rem(gb + j, n_b) for j in range(1, n_b)]

    def target(side):
        axis, up = side
        return {axis: place[axis] + (1 if up else -1)}

    barrier = pltpu.get_barrier_semaphore()
    partners = n_b - 1
    for side in sides:
        partners = partners + has[side].astype(jnp.int32)

        @pl.when(has[side])
        def _():
            pl.semaphore_signal(barrier, inc=1, device_id=target(side), device_id_type=MESH)

    for peer in peers:
        pl.semaphore_signal(barrier, inc=1, device_id={"band": peer}, device_id_type=MESH)
    orb_in = pltpu.make_async_copy(orb_hbm, orb_ref, in_sem.at[0])
    orb_in.start()
    ext_in = pltpu.make_async_copy(ext_hbm, ext_ref, in_sem.at[1])
    ext_in.start()

    chunks = max(1, min(6, ny // 2))
    x_cuts = [(j * (ny // chunks), ny // chunks + (ny % chunks if j == chunks - 1 else 0)) for j in range(chunks)]
    y_cuts = [(0, 2), (nx - 2, 2), (2, nx - 4)]
    d_cuts = [(0, 2), (ny - 2, 2), (2, ny - 4)]
    order = sorted(range(chunks), key=lambda j: 0 if j in (0, chunks - 1) else 1)
    sems = {"gx": (x_send, x_recv), "gy": (y_send, y_recv)}

    def cells(axis, edge, piece):
        if axis == "gx":
            return pl.ds(edge, 2), pl.ds(2 + x_cuts[piece][0], x_cuts[piece][1])
        return pl.ds(2 + y_cuts[piece][0], y_cuts[piece][1]), pl.ds(edge, 2)

    def send_copy(step, side, piece):
        axis, up = side
        extent = nx if axis == "gx" else ny
        src = terms[step].at[cells(axis, extent if up else 2, piece)]
        return pltpu.make_async_remote_copy(
            src_ref=src,
            dst_ref=terms[step].at[cells(axis, 0 if up else extent + 2, piece)],
            send_sem=sems[axis][0].at[step, up, piece],
            recv_sem=sems[axis][1].at[step, 1 - up, piece],
            device_id=target(side),
            device_id_type=MESH,
        )

    def start(step, side, piece):
        @pl.when(has[side])
        def _():
            send_copy(step, side, piece).start()

    def await_piece(step, side, piece):
        axis, up = side
        extent = nx if axis == "gx" else ny

        @pl.when(has[side])
        def _():
            land = terms[step].at[cells(axis, extent + 2 if up else 0, piece)]
            pltpu.make_async_remote_copy(
                src_ref=land,
                dst_ref=land,
                send_sem=sems[axis][0].at[step, up, piece],
                recv_sem=sems[axis][1].at[step, up, piece],
                device_id=target(side),
                device_id_type=MESH,
            ).wait_recv()

    def density_copy(which, j, piece):
        rows = pl.ds(*d_cuts[piece])
        return pltpu.make_async_remote_copy(
            src_ref=density.at[which, 0, rows],
            dst_ref=density.at[which, n_b - 1 - j, rows],
            send_sem=d_send.at[which, j, piece],
            recv_sem=d_recv.at[which, n_b - 2 - j, piece],
            device_id={"band": peers[j]},
            device_id_type=MESH,
        )

    def start_density(which, piece):
        for j in range(n_b - 1):
            density_copy(which, j, piece).start()

    def finish_potential(which):
        for piece in range(3):
            rows = pl.ds(*d_cuts[piece])
            for slot in range(1, n_b):
                pltpu.make_async_remote_copy(
                    src_ref=density.at[which, slot, rows],
                    dst_ref=density.at[which, slot, rows],
                    send_sem=d_send.at[which, slot - 1, piece],
                    recv_sem=d_recv.at[which, slot - 1, piece],
                    device_id={"band": peers[slot - 1]},
                    device_id_type=MESH,
                ).wait_recv()
        total = density[which, 0]
        for slot in range(1, n_b):
            total = total + density[which, slot]
        pot = ext_ref[...] - exchange_coef * cube_root(total)
        if which == 1:
            pot_ref[...] = pot
        wide = pot - 1.5 * centre_weight
        for y in range(ny):
            for x in range(nx):
                pot_wide[x, y] = jnp.broadcast_to(wide[y, x : x + 1], (nf, nz))

    for side in sides:
        axis, up = side

        @pl.when(jnp.logical_not(has[side]))
        def _():
            for step in range(8):
                if axis == "gx":
                    shape = (2, ny, nf, nz)
                    terms[step][pl.ds(nx + 2 if up else 0, 2), pl.ds(2, ny)] = jnp.zeros(shape, jnp.float32)
                else:
                    shape = (nx, 2, nf, nz)
                    terms[step][pl.ds(2, nx), pl.ds(ny + 2 if up else 0, 2)] = jnp.zeros(shape, jnp.float32)

    orb_in.wait()
    for y in range(ny):
        block = orb_ref[:, y]
        terms[0][pl.ds(2, nx), y + 2] = jnp.swapaxes(block, 0, 1)
        density[0, 0, y] = jnp.sum(block * block, axis=0)
    pl.semaphore_wait(barrier, partners)
    for j in order:
        for up in (0, 1):
            start(0, ("gx", up), j)
    for piece in range(3):
        for up in (0, 1):
            start(0, ("gy", up), piece)
    for piece in range(3):
        start_density(0, piece)
    ext_in.wait()

    lane = lax.broadcasted_iota(jnp.int32, (nf, nz), 1)
    near = -0.5 * near_weight
    far = -0.5 * far_weight
    below1 = jnp.where(lane >= 1, near, 0.0)
    above1 = jnp.where(lane < nz - 1, near, 0.0)
    below2 = jnp.where(lane >= 2, far, 0.0)
    above2 = jnp.where(lane < nz - 2, far, 0.0)
    half = nf // 2
    field = lax.broadcasted_iota(jnp.int32, (nf, nz), 0)
    turn_sign = jnp.where(field < half, 1.0, -1.0)

    def turned(v):
        return jnp.concatenate([v[half:], v[:half]], axis=0) * turn_sign

    def image(step, x, y):
        t = terms[step]
        c = t[x + 2, y + 2]
        one = (t[x + 1, y + 2] + t[x + 3, y + 2]) + (
            t[x + 2, y + 1] + t[x + 2, y + 3]
        )
        two = (t[x, y + 2] + t[x + 4, y + 2]) + (
            t[x + 2, y] + t[x + 2, y + 4]
        )
        total = pot_wide[x, y] * c + near * one + far * two
        total = total + pltpu.roll(c, 1, 1) * below1 + pltpu.roll(c, nz - 1, 1) * above1
        return total + (pltpu.roll(c, 2, 1) * below2 + pltpu.roll(c, nz - 2, 1) * above2)

    def combine(parts, s):
        even = parts[0] + (-(s**2) / 2) * parts[2] + (s**4 / 24) * parts[4]
        odd = s * parts[1] + (-(s**3) / 6) * parts[3]
        return even + turned(odd)

    def advance(step, xs, ys):
        at = [(x, y) for x in xs for y in ys]
        new = [image(step, x, y) for x, y in at]
        if step % 4 < 3:
            for (x, y), value in zip(at, new):
                terms[step + 1][x + 2, y + 2] = value
            return
        parts = [[terms[step - 3 + k][x + 2, y + 2] for k in range(4)] + [value] for (x, y), value in zip(at, new)]
        halves = [combine(part, step_length / 2) for part in parts]
        if step == 7:
            for (x, y), value in zip(at, halves):
                out_ref[x, y] = value
            return
        predicted = [combine(part, step_length) for part in parts]
        squares = [jnp.sum(value * value, axis=0, keepdims=True) for value in predicted]
        for (x, y), value, square in zip(at, halves, squares):
            terms[4][x + 2, y + 2] = value
            density[1, 0, y, pl.ds(x, 1)] = square

    rim = [0, 1, nx - 2, nx - 1]
    for step in range(8):
        if step % 4 == 0:
            finish_potential(step // 4)
        for j in order:
            edges = [("gy", up) for up, at in ((0, 0), (1, chunks - 1)) if at == j]
            for up in (0, 1):
                await_piece(step, ("gx", up), j)
            for side in edges:
                await_piece(step, side, 0)
                await_piece(step, side, 1)
            advance(step, rim, range(x_cuts[j][0], sum(x_cuts[j])))
            if step < 7:
                for up in (0, 1):
                    start(step + 1, ("gx", up), j)
                for side in edges:
                    start(step + 1, side, 0)
                    start(step + 1, side, 1)
        await_piece(step, ("gy", 0), 2)
        await_piece(step, ("gy", 1), 2)
        advance(step, range(2, nx - 2), [0, 1, ny - 2, ny - 1])
        if step < 7:
            start(step + 1, ("gy", 0), 2)
            start(step + 1, ("gy", 1), 2)
        if step == 3:
            start_density(1, 0)
            start_density(1, 1)
        for x in range(2, nx - 2):
            advance(step, [x], range(2, ny - 2))
        if step == 3:
            start_density(1, 2)

    for step in range(8):
        for side in sides:

            @pl.when(has[side])
            def _():
                for piece in range(chunks if side[0] == "gx" else 3):
                    send_copy(step, side, piece).wait_send()

    for which in (0, 1):
        for j in range(n_b - 1):
            for piece in range(3):
                density_copy(which, j, piece).wait_send()


def body(counts, orbitals, external):
    parts, bands, nx, ny, nz = orbitals.shape
    nf = parts * bands
    fields = jnp.transpose(orbitals.reshape(nf, nx, ny, nz), (0, 2, 1, 3))
    n_b = counts[2]
    dma = pltpu.SemaphoreType.DMA
    result, potential = pl.pallas_call(
        functools.partial(kernel, counts),
        out_shape=(
            jax.ShapeDtypeStruct((nx, ny, nf, nz), jnp.float32),
            jax.ShapeDtypeStruct((ny, nx, nz), jnp.float32),
        ),
        in_specs=[pl.BlockSpec(memory_space=pl.ANY)] * 2,
        out_specs=(pl.BlockSpec(memory_space=pltpu.VMEM),) * 2,
        scratch_shapes=[
            *[pltpu.VMEM((nx + 4, ny + 4, nf, nz), jnp.float32)] * 8,
            pltpu.VMEM((nf, ny, nx, nz), jnp.float32),
            pltpu.VMEM((ny, nx, nz), jnp.float32),
            pltpu.VMEM((nx, ny, nf, nz), jnp.float32),
            pltpu.VMEM((2, n_b, ny, nx, nz), jnp.float32),
            dma((2,)),
            dma((8, 2, 6)),
            dma((8, 2, 6)),
            dma((8, 2, 3)),
            dma((8, 2, 3)),
            dma((2, n_b - 1, 3)),
            dma((2, n_b - 1, 3)),
        ],
        compiler_params=pltpu.CompilerParams(
            collective_id=0, has_side_effects=True, vmem_limit_bytes=40 * 1024 * 1024
        ),
    )(fields, jnp.swapaxes(external, 0, 1))
    result = jnp.transpose(result, (2, 0, 1, 3)).reshape(orbitals.shape)
    return (result, jnp.swapaxes(potential, 0, 1))


def solution(mesh):
    counts = (mesh.shape["gx"], mesh.shape["gy"], mesh.shape["band"])
    in_specs = (P(None, "band", "gx", "gy", None), P("gx", "gy", None))
    out_specs = (P(None, "band", "gx", "gy", None), P("gx", "gy", None))
    return jax.shard_map(
        functools.partial(body, counts), mesh=mesh, in_specs=in_specs, out_specs=out_specs, check_vma=False
    )
```

```python
import functools

import jax
import jax.numpy as jnp
from jax import lax
from jax.experimental import pallas as pl
from jax.experimental.pallas import tpu as pltpu
from jax.sharding import PartitionSpec as P

step_length = 0.15
exchange_coef = 0.7386
centre_weight = -2.5
near_weight = 4.0 / 3.0
far_weight = -1.0 / 12.0
MESH = pl.DeviceIdType.MESH


def cube_root(d):
    guess = jnp.exp(jnp.log(d) * (1.0 / 3.0))
    better = guess - (guess - d / (guess * guess)) * (1.0 / 3.0)
    return jnp.where(d > 1e-30, better, guess)


def kernel(counts, orb_hbm, ext_hbm, out_ref, pot_ref, *scratch):
    terms = scratch[:8]
    orb_ref, ext_ref, pot_wide, density, in_sem, x_send, x_recv, y_send, y_recv, d_send, d_recv = scratch[8:]
    n_x, n_y, n_b = counts
    nf, ny, nx, nz = orb_ref.shape
    gx = lax.axis_index("gx")
    gy = lax.axis_index("gy")
    gb = lax.axis_index("band")
    has = {
        ("gx", 0): gx > 0,
        ("gx", 1): gx < n_x - 1,
        ("gy", 0): gy > 0,
        ("gy", 1): gy < n_y - 1,
    }
    place = {"gx": gx, "gy": gy}
    if n_x == 2:
        x_sides = [("gx", 1 - gx)]
    else:
        x_sides = [("gx", 0), ("gx", 1)]
    y_sides = [("gy", 0), ("gy", 1)]
    sides = [("gx", 0), ("gx", 1)] + y_sides
    peers = [lax.rem(gb + j, n_b) for j in range(1, n_b)]

    def target(side):
        axis, up = side
        return {axis: place[axis] + (2 * up - 1)}

    barrier = pltpu.get_barrier_semaphore()
    partners = n_b - 1
    for side in sides:
        partners = partners + has[side].astype(jnp.int32)

        @pl.when(has[side])
        def _():
            pl.semaphore_signal(barrier, inc=1, device_id=target(side), device_id_type=MESH)

    for peer in peers:
        pl.semaphore_signal(barrier, inc=1, device_id={"band": peer}, device_id_type=MESH)
    orb_in = pltpu.make_async_copy(orb_hbm, orb_ref, in_sem.at[0])
    orb_in.start()
    ext_in = pltpu.make_async_copy(ext_hbm, ext_ref, in_sem.at[1])
    ext_in.start()

    chunks = max(1, min(6, ny // 2))
    x_cuts = [(j * (ny // chunks), ny // chunks + (ny % chunks if j == chunks - 1 else 0)) for j in range(chunks)]
    mid = (nx - 4) // 2
    y_cuts = [(0, 2), (nx - 2, 2), (2, mid), (2 + mid, nx - 4 - mid)]
    d_cuts = [(0, 2), (ny - 2, 2), (2, ny - 4)]
    order = sorted(range(chunks), key=lambda j: 0 if j in (0, chunks - 1) else 1)
    sems = {"gx": (x_send, x_recv), "gy": (y_send, y_recv)}

    def cells(axis, edge, piece):
        if axis == "gx":
            return pl.ds(edge, 2), pl.ds(2 + x_cuts[piece][0], x_cuts[piece][1])
        return pl.ds(2 + y_cuts[piece][0], y_cuts[piece][1]), pl.ds(edge, 2)

    def pick(up, high, low):
        if isinstance(up, int):
            return high if up else low
        return low + up * (high - low)

    def send_copy(step, side, piece):
        axis, up = side
        extent = nx if axis == "gx" else ny
        return pltpu.make_async_remote_copy(
            src_ref=terms[step].at[cells(axis, pick(up, extent, 2), piece)],
            dst_ref=terms[step].at[cells(axis, pick(up, 0, extent + 2), piece)],
            send_sem=sems[axis][0].at[step, up, piece],
            recv_sem=sems[axis][1].at[step, 1 - up, piece],
            device_id=target(side),
            device_id_type=MESH,
        )

    def recv_copy(step, side, piece):
        axis, up = side
        extent = nx if axis == "gx" else ny
        land = terms[step].at[cells(axis, pick(up, extent + 2, 0), piece)]
        return pltpu.make_async_remote_copy(
            src_ref=land,
            dst_ref=land,
            send_sem=sems[axis][0].at[step, up, piece],
            recv_sem=sems[axis][1].at[step, up, piece],
            device_id=target(side),
            device_id_type=MESH,
        )

    def each(side, act):
        if side[0] == "gx" and n_x == 2:
            act()
        else:
            pl.when(has[side])(act)

    def start(step, side, pieces):
        def act():
            for piece in pieces:
                send_copy(step, side, piece).start()

        each(side, act)

    def await_pieces(step, side, pieces):
        def act():
            for piece in pieces:
                recv_copy(step, side, piece).wait_recv()

        each(side, act)

    def density_copy(which, j, piece):
        rows = pl.ds(*d_cuts[piece])
        return pltpu.make_async_remote_copy(
            src_ref=density.at[which, 0, rows],
            dst_ref=density.at[which, n_b - 1 - j, rows],
            send_sem=d_send.at[which, j, piece],
            recv_sem=d_recv.at[which, n_b - 2 - j, piece],
            device_id={"band": peers[j]},
            device_id_type=MESH,
        )

    def start_density(which, piece):
        for j in range(n_b - 1):
            density_copy(which, j, piece).start()

    def finish_potential(which):
        for piece in range(3):
            rows = pl.ds(*d_cuts[piece])
            for slot in range(1, n_b):
                pltpu.make_async_remote_copy(
                    src_ref=density.at[which, slot, rows],
                    dst_ref=density.at[which, slot, rows],
                    send_sem=d_send.at[which, slot - 1, piece],
                    recv_sem=d_recv.at[which, slot - 1, piece],
                    device_id={"band": peers[slot - 1]},
                    device_id_type=MESH,
                ).wait_recv()
        total = density[which, 0]
        for slot in range(1, n_b):
            total = total + density[which, slot]
        pot = ext_ref[...] - exchange_coef * cube_root(total)
        if which == 1:
            pot_ref[...] = pot
        wide = pot - 1.5 * centre_weight
        for y in range(ny):
            for x in range(nx):
                pot_wide[x, y] = jnp.broadcast_to(wide[y, x : x + 1], (nf, nz))

    for side in sides:
        axis, up = side

        @pl.when(jnp.logical_not(has[side]))
        def _():
            for step in range(8):
                if axis == "gx":
                    shape = (2, ny, nf, nz)
                    terms[step][pl.ds(nx + 2 if up else 0, 2), pl.ds(2, ny)] = jnp.zeros(shape, jnp.float32)
                else:
                    shape = (nx, 2, nf, nz)
                    terms[step][pl.ds(2, nx), pl.ds(ny + 2 if up else 0, 2)] = jnp.zeros(shape, jnp.float32)

    orb_in.wait()
    for y in range(ny):
        block = orb_ref[:, y]
        terms[0][pl.ds(2, nx), y + 2] = jnp.swapaxes(block, 0, 1)
        density[0, 0, y] = jnp.sum(block * block, axis=0)
    pl.semaphore_wait(barrier, partners)
    for side in x_sides:
        start(0, side, order)
    for side in y_sides:
        start(0, side, range(4))
    for piece in range(3):
        start_density(0, piece)
    ext_in.wait()

    lane = lax.broadcasted_iota(jnp.int32, (nf, nz), 1)
    near = -0.5 * near_weight
    far = -0.5 * far_weight
    below1 = jnp.where(lane >= 1, near, 0.0)
    above1 = jnp.where(lane < nz - 1, near, 0.0)
    below2 = jnp.where(lane >= 2, far, 0.0)
    above2 = jnp.where(lane < nz - 2, far, 0.0)
    half = nf // 2
    field = lax.broadcasted_iota(jnp.int32, (nf, nz), 0)
    turn_sign = jnp.where(field < half, 1.0, -1.0)

    def turned(v):
        return jnp.concatenate([v[half:], v[:half]], axis=0) * turn_sign

    def image(step, x, y):
        t = terms[step]
        c = t[x + 2, y + 2]
        one = (t[x + 1, y + 2] + t[x + 3, y + 2]) + (
            t[x + 2, y + 1] + t[x + 2, y + 3]
        )
        two = (t[x, y + 2] + t[x + 4, y + 2]) + (
            t[x + 2, y] + t[x + 2, y + 4]
        )
        total = pot_wide[x, y] * c + near * one + far * two
        total = total + pltpu.roll(c, 1, 1) * below1 + pltpu.roll(c, nz - 1, 1) * above1
        return total + (pltpu.roll(c, 2, 1) * below2 + pltpu.roll(c, nz - 2, 1) * above2)

    def combine(parts, s):
        even = parts[0] + (-(s**2) / 2) * parts[2] + (s**4 / 24) * parts[4]
        odd = s * parts[1] + (-(s**3) / 6) * parts[3]
        return even + turned(odd)

    def advance(step, xs, ys):
        at = [(x, y) for x in xs for y in ys]
        new = [image(step, x, y) for x, y in at]
        if step % 4 < 3:
            for (x, y), value in zip(at, new):
                terms[step + 1][x + 2, y + 2] = value
            return
        parts = [[terms[step - 3 + k][x + 2, y + 2] for k in range(4)] + [value] for (x, y), value in zip(at, new)]
        halves = [combine(part, step_length / 2) for part in parts]
        if step == 7:
            for (x, y), value in zip(at, halves):
                out_ref[x, y] = value
            return
        predicted = [combine(part, step_length) for part in parts]
        squares = [jnp.sum(value * value, axis=0, keepdims=True) for value in predicted]
        for (x, y), value, square in zip(at, halves, squares):
            terms[4][x + 2, y + 2] = value
            density[1, 0, y, pl.ds(x, 1)] = square

    rim = [0, 1, nx - 2, nx - 1]
    for step in range(8):
        if step % 4 == 0:
            finish_potential(step // 4)
        for n, j in enumerate(order):
            edges = [("gy", up) for up, at in ((0, 0), (1, chunks - 1)) if at == j]
            for side in x_sides:
                await_pieces(step, side, [j])
            for side in edges:
                await_pieces(step, side, [0, 1])
            advance(step, rim, range(x_cuts[j][0], sum(x_cuts[j])))
            if step < 7:
                for side in x_sides:
                    start(step + 1, side, [j])
                for side in edges:
                    start(step + 1, side, [0, 1])
            if n == min(1, chunks - 1):
                for piece in (2, 3):
                    for side in y_sides:
                        await_pieces(step, side, [piece])
                    advance(step, range(y_cuts[piece][0], sum(y_cuts[piece])), [0, 1, ny - 2, ny - 1])
                    if step < 7:
                        for side in y_sides:
                            start(step + 1, side, [piece])
                if step == 3:
                    start_density(1, 0)
                    start_density(1, 1)
        for x in range(2, nx - 2):
            advance(step, [x], range(2, ny - 2))
        if step == 3:
            start_density(1, 2)

    for side in x_sides + y_sides:

        def drain():
            for step in range(8):
                for piece in range(chunks if side[0] == "gx" else 4):
                    send_copy(step, side, piece).wait_send()

        each(side, drain)

    for which in (0, 1):
        for j in range(n_b - 1):
            for piece in range(3):
                density_copy(which, j, piece).wait_send()


def body(counts, orbitals, external):
    parts, bands, nx, ny, nz = orbitals.shape
    nf = parts * bands
    fields = jnp.transpose(orbitals.reshape(nf, nx, ny, nz), (0, 2, 1, 3))
    n_b = counts[2]
    dma = pltpu.SemaphoreType.DMA
    result, potential = pl.pallas_call(
        functools.partial(kernel, counts),
        out_shape=(
            jax.ShapeDtypeStruct((nx, ny, nf, nz), jnp.float32),
            jax.ShapeDtypeStruct((ny, nx, nz), jnp.float32),
        ),
        in_specs=[pl.BlockSpec(memory_space=pltpu.HBM)] * 2,
        out_specs=(pl.BlockSpec(memory_space=pltpu.VMEM),) * 2,
        scratch_shapes=[
            *[pltpu.VMEM((nx + 4, ny + 4, nf, nz), jnp.float32)] * 8,
            pltpu.VMEM((nf, ny, nx, nz), jnp.float32),
            pltpu.VMEM((ny, nx, nz), jnp.float32),
            pltpu.VMEM((nx, ny, nf, nz), jnp.float32),
            pltpu.VMEM((2, n_b, ny, nx, nz), jnp.float32),
            dma((2,)),
            dma((8, 2, 6)),
            dma((8, 2, 6)),
            dma((8, 2, 4)),
            dma((8, 2, 4)),
            dma((2, n_b - 1, 3)),
            dma((2, n_b - 1, 3)),
        ],
        compiler_params=pltpu.CompilerParams(
            collective_id=0, has_side_effects=True, vmem_limit_bytes=40 * 1024 * 1024
        ),
    )(fields, jnp.swapaxes(external, 0, 1))
    result = jnp.transpose(result, (2, 0, 1, 3)).reshape(orbitals.shape)
    return (result, jnp.swapaxes(potential, 0, 1))


def solution(mesh):
    counts = (mesh.shape["gx"], mesh.shape["gy"], mesh.shape["band"])
    in_specs = (P(None, "band", "gx", "gy", None), P("gx", "gy", None))
    out_specs = (P(None, "band", "gx", "gy", None), P("gx", "gy", None))
    return jax.shard_map(
        functools.partial(body, counts), mesh=mesh, in_specs=in_specs, out_specs=out_specs, check_vma=False
    )
```
